32 devices in a mesh: seq: 4 (over y, x), head: 8 (over z, core).
Axes of the slice: x: 2, y: 2, z: 4, core: 2. Of those that a mesh axis runs over, the one named last changes fastest.
Arguments:
- queries: bfloat16 [8192, 4096], P(('seq', 'head')), may hold values from -6 to 6
- key_vectors: bfloat16 [8192, 4096], P(('seq', 'head')), may hold values from -0.375 to 0.375
- values: bfloat16 [8192, 8192], P(('seq', 'head')), may hold values from -6 to 6
- decay_log: bfloat16 [8192, 16], P(('seq', 'head')), may hold values from -0.8 to 0, as said below
- gate_input: bfloat16 [8192, 8192], P(('seq', 'head')), may hold values from -6 to 6
Outputs:
- retention_out: bfloat16 [8192, 8192], P(('seq', 'head'))
The draws below stay inside these ranges and needn't reach their ends.
Inputs may be any that keep to these rules, and one draw needn't show every extreme that they name: `decay_log`: every entry is negative.
All inputs are finite; a program needn't handle non-finite values.
Results may differ from the reference program's by a relative error of at most 0.0063.
Values may be sent and summed in bfloat16 or wider, within the bound.
A program may use at most 128 MiB of HBM per device.

```python
import math
import jax
import jax.numpy as jnp
from jax import lax

RETAIN_HEADS = 16
DK = 256
DV = 512
BLOCK = 512
DOC_POSITIONS = 8192


def draw_decay_log(key, part):
    key_kind, key_slow, key_fast, key_rough, key_location, key_magnitude, key_medium = jax.random.split(key, 7)
    fast_count = 4
    medium_count = 4
    medium_low = math.log(1.0 / 600.0)
    medium_high = math.log(1.0 / 300.0)
    head_rank = jax.random.permutation(key_kind, jnp.arange(RETAIN_HEADS, dtype=jnp.int32))
    fast_heads = head_rank < fast_count
    medium_heads = jnp.logical_and(head_rank >= fast_count, head_rank < fast_count + medium_count)
    slow_rate = jnp.exp(jax.random.uniform(key_slow, (RETAIN_HEADS,), jnp.float32, math.log(0.2), math.log(0.5))) / DOC_POSITIONS
    fast_rate = jnp.exp(jax.random.uniform(key_fast, (RETAIN_HEADS,), jnp.float32, math.log(1.0 / 50.0), math.log(1.0 / 30.0)))
    medium_rate = jnp.exp(jax.random.uniform(key_medium, (RETAIN_HEADS,), jnp.float32, medium_low, medium_high))
    head_decay_rate = jnp.where(fast_heads, fast_rate, jnp.where(medium_heads, medium_rate, slow_rate))
    jaggedness = jnp.exp(jax.random.uniform(key_rough, (DOC_POSITIONS, RETAIN_HEADS), jnp.float32, math.log(0.5), math.log(2.0)))
    key_first, key_gap = jax.random.split(key_location)
    first_spot = jax.random.randint(key_first, (RETAIN_HEADS,), 0, DOC_POSITIONS)
    spot_gap = jax.random.randint(key_gap, (RETAIN_HEADS,), 0, DOC_POSITIONS - 1)
    second_spot = (first_spot + 1 + spot_gap) % DOC_POSITIONS
    spike_magnitude = jax.random.uniform(key_magnitude, (2, RETAIN_HEADS), jnp.float32, math.log(0.5), math.log(0.8))
    token_offset = jnp.arange(DOC_POSITIONS)[:, None]
    decay_spikes = jnp.where(token_offset == first_spot[None, :], spike_magnitude[0][None, :], 0.0)
    decay_spikes = decay_spikes + jnp.where(token_offset == second_spot[None, :], spike_magnitude[1][None, :], 0.0)
    return (decay_spikes - head_decay_rate[None, :] * jaggedness).astype(jnp.bfloat16)


def block_scale(key, extent, cuts, low, high):
    level, own = 1.0, jax.random.fold_in(key, 6)
    for dim, shards_of in cuts:
        heights = jnp.exp(jax.random.uniform(jax.random.fold_in(own, dim), (shards_of,), jnp.float32, low / len(cuts), high / len(cuts)))
        level = level * jnp.repeat(heights, extent[dim] // shards_of).reshape([-1 if axis == dim else 1 for axis in range(len(extent))])
    return level


def bell_draw(own_key, shape, deviation, reach, shards=(), held_as=jnp.bfloat16):
    factor_of = block_scale(own_key, shape, shards, -0.22, 0.18) if shards else 1.0
    array = jax.random.normal(own_key, shape, jnp.float32) * deviation * factor_of
    return jnp.minimum(jnp.maximum(array, -reach), reach).astype(held_as)


def setup_inputs(seed: int = 0) -> dict:
    key_of = jax.random.split(jax.random.key(seed), 6)
    return {
        "queries": bell_draw(key_of[0], (DOC_POSITIONS, RETAIN_HEADS * DK), 1.0, 6.0, ((0, 32),)),
        "key_vectors": bell_draw(key_of[1], (DOC_POSITIONS, RETAIN_HEADS * DK), 0.0625, 0.375, ((0, 32),)),
        "values": bell_draw(key_of[2], (DOC_POSITIONS, RETAIN_HEADS * DV), 1.0, 6.0, ((0, 32),)),
        "decay_log": draw_decay_log(jax.random.fold_in(key_of[5], 71), 0),
        "gate_input": bell_draw(key_of[4], (DOC_POSITIONS, RETAIN_HEADS * DV), 1.0, 6.0, ((0, 32),)),
    }


def reference(queries, key_vectors, values, decay_log, gate_input):
    blocks = DOC_POSITIONS // BLOCK
    query_blocks = queries.reshape(blocks, BLOCK, RETAIN_HEADS, DK)
    key_blocks = key_vectors.reshape(blocks, BLOCK, RETAIN_HEADS, DK)
    value_blocks = values.reshape(blocks, BLOCK, RETAIN_HEADS, DV)
    decay_blocks = decay_log.astype(jnp.float32).reshape(blocks, BLOCK, RETAIN_HEADS)
    causal = jnp.arange(BLOCK)[:, None] >= jnp.arange(BLOCK)[None, :]

    def advance(carried_state, pieces):
        query_block, key_block, value_block, decay_block = pieces
        running = jnp.cumsum(decay_block, axis=0)
        block_decay = running[-1]
        faded = (key_block.astype(jnp.float32) * jnp.exp(block_decay[None, :] - running)[:, :, None]).astype(jnp.bfloat16)
        state_low = carried_state.astype(jnp.bfloat16)
        spread = running.T[:, :, None] - running.T[:, None, :]
        factor = jnp.exp(jnp.where(causal[None], spread, -jnp.inf))
        scores = jnp.einsum('ihd,jhd->hij', query_block.astype(jnp.float32), key_block.astype(jnp.float32))
        weights = (scores * factor).astype(jnp.bfloat16)
        within = jnp.einsum('hij,jhw->ihw', weights.astype(jnp.float32), value_block.astype(jnp.float32))
        across = jnp.einsum('ihd,hdw->ihw', query_block.astype(jnp.float32), state_low.astype(jnp.float32))
        across = across * jnp.exp(running)[:, :, None]
        retained = (within + across).astype(jnp.bfloat16)
        additions = jnp.einsum('jhd,jhw->hdw', faded.astype(jnp.float32), value_block.astype(jnp.float32))
        updated = jnp.exp(block_decay)[:, None, None] * carried_state + additions
        return (updated, retained)
    initial = jnp.zeros((RETAIN_HEADS, DK, DV), jnp.float32)
    unused, retained = lax.scan(advance, initial, (query_blocks, key_blocks, value_blocks, decay_blocks))
    retained = retained.reshape(DOC_POSITIONS, RETAIN_HEADS, DV).astype(jnp.float32)
    average = lax.optimization_barrier(jnp.mean(retained, axis=2, keepdims=True))
    centered = retained - average
    variance = lax.optimization_barrier(jnp.mean(centered * centered, axis=2, keepdims=True))
    normed = centered / jnp.sqrt(variance + 1e-06)
    gated = jax.nn.silu(gate_input.astype(jnp.float32).reshape(DOC_POSITIONS, RETAIN_HEADS, DV)) * normed
    return gated.astype(jnp.bfloat16).reshape(DOC_POSITIONS, RETAIN_HEADS * DV)
```

```python
import functools

import jax
import jax.numpy as jnp
from jax import lax
from jax.experimental import pallas as pl
from jax.experimental.pallas import tpu as pltpu
from jax.sharding import PartitionSpec as P

MESH = pl.DeviceIdType.MESH
F32 = jnp.float32
BF16 = jnp.bfloat16
LAG = 2
CUTS = 2


def dot(a, b, dims):
    return lax.dot_general(a, b, (dims, ((), ())), preferred_element_type=F32)


def wide(column, times):
    return jnp.concatenate([column] * times, axis=1)


def retention_kernel(
    seqs, chips, heads, q_ref, k_ref, v_ref, dec_ref, out_ref,
    qbuf, kbuf, vbuf, decbuf, runcol, runrow, gath, coef, tri,
    abuf, ebuf, within, slow, retbuf, sbuf, rbuf, supb, rupb, sdnb, rdnb,
    xs, xr, loc, gs, gr, ss, sr, ups, upr, dns, dnr, rets, retr, retl,
):
    s = lax.axis_index("seq")
    h = lax.axis_index("head")
    c = lax.rem(h, 2)
    z = h // 2
    steps = seqs.bit_length() - 1
    rows = q_ref.shape[0]
    block = 2 * rows
    dk = qbuf.shape[2]
    dv = vbuf.shape[2]
    blocks = seqs * chips
    me = s * chips + z
    units = heads * CUTS
    urows = dk // CUTS
    mate = {"seq": s, "head": h + 1 - 2 * c}

    def spot(b):
        return {"seq": b // chips, "head": 2 * lax.rem(b, chips) + c}

    barrier = pltpu.get_barrier_semaphore()
    pl.semaphore_signal(barrier, inc=1, device_id=mate, device_id_type=MESH)

    def greet(o, _):
        pl.semaphore_signal(
            barrier, inc=1, device_id=spot(lax.rem(me + o, blocks)), device_id_type=MESH
        )
        return 0

    lax.fori_loop(1, blocks, greet, 0)
    pl.semaphore_wait(barrier, blocks)

    mine = pl.ds(pl.multiple_of(c * rows, rows), rows)

    def swap(kind, i):
        if kind == 3:
            source, target = dec_ref.at[1 - c], decbuf.at[mine]
        else:
            ref, buf = ((k_ref, kbuf), (v_ref, vbuf), (q_ref, qbuf))[kind]
            width = buf.shape[2]
            col = pl.multiple_of(((1 - c) * heads + i) * width, width)
            source, target = ref.at[:, pl.ds(col, width)], buf.at[i, mine, :]
        return pltpu.make_async_remote_copy(
            src_ref=source, dst_ref=target, send_sem=xs.at[kind, i], recv_sem=xr.at[kind, i],
            device_id=mate, device_id_type=MESH,
        )

    def keep(kind, i):
        if kind == 3:
            source, target = dec_ref.at[c], decbuf.at[mine]
        else:
            ref, buf = ((k_ref, kbuf), (v_ref, vbuf), (q_ref, qbuf))[kind]
            width = buf.shape[2]
            col = pl.multiple_of((c * heads + i) * width, width)
            source, target = ref.at[:, pl.ds(col, width)], buf.at[i, mine, :]
        return pltpu.make_async_copy(source, target, loc.at[kind, i])

    swap(3, 0).start()
    keep(3, 0).start()

    def launch(i, _):
        for kind in (0, 1):
            swap(kind, i).start()
            keep(kind, i).start()
        return 0

    lax.fori_loop(0, heads, launch, 0)

    def launch_q(i, _):
        swap(2, i).start()
        keep(2, i).start()
        return 0

    lax.fori_loop(0, heads, launch_q, 0)

    row_id = lax.broadcasted_iota(jnp.int32, (block, block), 0)
    col_id = lax.broadcasted_iota(jnp.int32, (block, block), 1)
    tri[...] = jnp.where(row_id >= col_id, 1.0, 0.0).astype(BF16)
    keep(3, 0).wait()
    swap(3, 0).wait_recv()
    dec = decbuf[...]
    running = dot(tri[...], dec, ((1,), (0,)))
    run_rows = dot(dec, tri[...], ((0,), (1,)))
    runrow[...] = run_rows[:heads, :][:, None, :]
    gath[me] = dot(dec, jnp.ones((block, dv), BF16), ((0,), (0,)))[:heads, :]
    for i in range(heads):
        runcol[i] = jnp.broadcast_to(running[:, i : i + 1], (block, 128))

    def tell(o, where):
        return pltpu.make_async_remote_copy(
            src_ref=gath.at[me], dst_ref=gath.at[where], send_sem=gs.at[o], recv_sem=gr.at[o],
            device_id=spot(lax.rem(me + o, blocks)), device_id_type=MESH,
        )

    def tell_start(o, _):
        tell(o, me).start()
        return 0

    lax.fori_loop(1, blocks, tell_start, 0)

    def hop(k, u):
        other = s ^ (1 << k)
        return pltpu.make_async_remote_copy(
            src_ref=sbuf.at[k, u], dst_ref=rbuf.at[k, u], send_sem=ss.at[k, u],
            recv_sem=sr.at[k, u], device_id={"seq": other, "head": h}, device_id_type=MESH,
        )

    def up(u):
        return pltpu.make_async_remote_copy(
            src_ref=supb.at[u], dst_ref=rupb.at[u], send_sem=ups.at[u], recv_sem=upr.at[u],
            device_id={"seq": s, "head": lax.rem(h + 2, 2 * chips)}, device_id_type=MESH,
        )

    def down(u):
        return pltpu.make_async_remote_copy(
            src_ref=sdnb.at[u], dst_ref=rdnb.at[u], send_sem=dns.at[u], recv_sem=dnr.at[u],
            device_id={"seq": s, "head": lax.rem(h - 2 + 2 * chips, 2 * chips)},
            device_id_type=MESH,
        )

    def bit(k):
        return lax.rem(s // (1 << k), 2)

    def sends(k):
        return True if k < steps - 1 else bit(k) == 0

    def gets(k):
        return True if k < steps - 1 else bit(k) == 1

    def state(i, _):
        for kind in (0, 1):
            keep(kind, i).wait()
            swap(kind, i).wait_recv()
        total = gath[me, pl.ds(i, 1), :][:, :128]
        fade = wide(jnp.exp(total - runcol[i]), dk // 128)
        faded = (kbuf[i].astype(F32) * fade).astype(BF16)
        for cut in range(CUTS):
            u = i * CUTS + cut
            part = dot(faded[:, cut * urows : (cut + 1) * urows], vbuf[i], ((0,), (0,)))
            abuf[u] = part
            if steps > 0:
                sbuf[0, u] = part.astype(BF16)

                @pl.when(sends(0))
                def _():
                    hop(0, u).start()

        return 0

    lax.fori_loop(0, heads, state, 0)

    def hear(o, _):
        tell(o, lax.rem(me - o + blocks, blocks)).wait_recv()
        return 0

    lax.fori_loop(1, blocks, hear, 0)

    def span(slot, lo, hi, live=None):
        total = lax.fori_loop(
            lo, hi, lambda b, acc: acc + gath[b], jnp.zeros((heads, dv), F32)
        )
        value = jnp.exp(total)
        if live is not None:
            value = value * live.astype(F32)
        coef[slot] = value

    def end(p, k):
        return p * chips + z + 1 if k == 0 else (p // (1 << k) + 1) * (1 << k) * chips

    for k in range(steps):
        other = s ^ (1 << k)
        span(3 * k, end(s, k), end(s, k + 1))
        span(3 * k + 1, end(other, k), end(s, k + 1))
        span(3 * k + 2, end(other, k), jnp.maximum(s * chips, end(other, k)), bit(k))
    base = 3 * steps
    span(base, me, me + 1)
    span(base + 1, s * chips, me + 1)
    span(base + 2, s * chips, me)

    @pl.when(z == 0)
    def _():
        rupb[...] = jnp.zeros(rupb.shape, BF16)

    @pl.when(z == chips - 1)
    def _():
        rdnb[...] = jnp.zeros(rdnb.shape, BF16)

    def scale(slot, u):
        return coef[slot, pl.ds(u // CUTS, 1), :]

    def when(live, u, fn):
        pl.when(jnp.logical_and(live, jnp.logical_and(u >= 0, u < units)))(lambda: fn(u))

    def step(t, _):
        for k in range(steps):

            def scan(u, k=k):
                @pl.when(gets(k))
                def _():
                    hop(k, u).wait_recv()
                    got = rbuf[k, u].astype(F32)
                    add = got * scale(3 * k + 2, u)
                    ebuf[u] = add if k == 0 else ebuf[u] + add
                    if k < steps - 1:
                        own = abuf[u] if k == 0 else sbuf[k, u].astype(F32)
                        sbuf[k + 1, u] = (
                            own * scale(3 * k, u) + got * scale(3 * k + 1, u)
                        ).astype(BF16)

                if k == 0 and steps == 1:

                    @pl.when(jnp.logical_not(gets(0)))
                    def _():
                        ebuf[u] = jnp.zeros((urows, dv), F32)

                if k < steps - 1:

                    @pl.when(sends(k + 1))
                    def _():
                        hop(k + 1, u).start()

            when(True, t - LAG * k, scan)
        if steps == 0:

            def blank(u):
                ebuf[u] = jnp.zeros((urows, dv), F32)

            when(True, t, blank)
        ready = t - LAG * max(steps - 1, 0)

        def rise(u):
            @pl.when(z > 0)
            def _():
                up(u).wait_recv()

            @pl.when(z < chips - 1)
            def _():
                supb[u] = (
                    rupb[u].astype(F32) * scale(base, u)
                    + abuf[u]
                    + scale(base + 1, u) * ebuf[u]
                ).astype(BF16)
                up(u).start()

        when(True, ready - LAG * z, rise)

        def sink(u):
            @pl.when(z < chips - 1)
            def _():
                down(u).wait_recv()

            @pl.when(z > 0)
            def _():
                sdnb[u] = (rdnb[u].astype(F32) + ebuf[u]).astype(BF16)
                down(u).start()

        when(True, ready - LAG * (chips - 1 - z), sink)

        def local(i):
            keep(2, i).wait()
            swap(2, i).wait_recv()
            scores = dot(qbuf[i], kbuf[i], ((1,), (1,)))
            spread = wide(runcol[i], block // 128) - runrow[i]
            row = lax.broadcasted_iota(jnp.int32, (block, block), 0)
            col = lax.broadcasted_iota(jnp.int32, (block, block), 1)
            factor = jnp.exp(jnp.where(row >= col, spread, -jnp.inf))
            weights = (scores * factor).astype(BF16)
            within[i] = dot(weights, vbuf[i], ((1,), (0,)))

        pl.when(t < heads)(lambda: local(t))

        def finish(u):
            i = u // CUTS
            start = rupb[u].astype(F32) + scale(base + 2, u) * (rdnb[u].astype(F32) + ebuf[u])
            slow[u] = start.astype(BF16)

            @pl.when(lax.rem(u, CUTS) == CUTS - 1)
            def _():
                low = slow[pl.ds(i * CUTS, CUTS)].reshape(dk, dv)
                across = dot(qbuf[i], low, ((1,), (0,)))
                across = across * wide(jnp.exp(runcol[i]), dv // 128)
                retbuf[i] = (within[i] + across).astype(BF16)
                give(i).start()
                stay(i).start()

        when(True, ready - LAG * jnp.maximum(z, chips - 1 - z), finish)
        return 0

    yours = pl.ds(pl.multiple_of((1 - c) * rows, rows), rows)

    def give(i):
        col = pl.multiple_of((c * heads + i) * dv, dv)
        return pltpu.make_async_remote_copy(
            src_ref=retbuf.at[i, yours, :], dst_ref=out_ref.at[:, pl.ds(col, dv)],
            send_sem=rets.at[i], recv_sem=retr.at[i], device_id=mate, device_id_type=MESH,
        )

    def take(i):
        col = pl.multiple_of(((1 - c) * heads + i) * dv, dv)
        return pltpu.make_async_remote_copy(
            src_ref=retbuf.at[i, yours, :], dst_ref=out_ref.at[:, pl.ds(col, dv)],
            send_sem=rets.at[i], recv_sem=retr.at[i], device_id=mate, device_id_type=MESH,
        )

    def stay(i):
        col = pl.multiple_of((c * heads + i) * dv, dv)
        return pltpu.make_async_copy(
            retbuf.at[i, mine, :], out_ref.at[:, pl.ds(col, dv)], retl.at[i]
        )

    total_steps = max(units + LAG * max(steps - 1, 0) + LAG * (chips - 1), heads)
    lax.fori_loop(0, total_steps, step, 0)

    swap(3, 0).wait_send()

    def close(i, _):
        for kind in range(3):
            swap(kind, i).wait_send()
        give(i).wait_send()
        take(i).wait_recv()
        stay(i).wait()
        return 0

    lax.fori_loop(0, heads, close, 0)

    def close_tell(o, _):
        tell(o, me).wait_send()
        return 0

    lax.fori_loop(1, blocks, close_tell, 0)

    def close_units(u, _):
        for k in range(steps):

            @pl.when(sends(k))
            def _():
                hop(k, u).wait_send()

        @pl.when(z < chips - 1)
        def _():
            up(u).wait_send()

        @pl.when(z > 0)
        def _():
            down(u).wait_send()

        return 0

    lax.fori_loop(0, units, close_units, 0)


def gate_kernel(ret_ref, gate_ref, out_ref):
    kept = ret_ref[...].astype(F32)
    centered = kept - jnp.mean(kept, axis=1, keepdims=True)
    variance = jnp.mean(centered * centered, axis=1, keepdims=True)
    normed = centered / jnp.sqrt(variance + 1e-06)
    gate = gate_ref[...].astype(F32)
    out_ref[...] = (jax.nn.silu(gate) * normed).astype(BF16)


def shards(seqs, groups, queries, key_vectors, values, decay_log, gate_input):
    rows, head_count = decay_log.shape
    heads = head_count // 2
    chips = groups // 2
    dk = queries.shape[1] // head_count
    dv = values.shape[1] // head_count
    block = 2 * rows
    blocks = seqs * chips
    units = heads * CUTS
    urows = dk // CUTS
    steps = seqs.bit_length() - 1
    hops = max(steps, 1)
    dec = jnp.pad(
        decay_log.reshape(rows, 2, heads).swapaxes(0, 1), ((0, 0), (0, 0), (0, 128 - heads))
    )
    hbm = pl.BlockSpec(memory_space=pl.ANY)
    dma = lambda *shape: pltpu.SemaphoreType.DMA(shape)
    retained = pl.pallas_call(
        functools.partial(retention_kernel, seqs, chips, heads),
        out_shape=jax.ShapeDtypeStruct(values.shape, BF16),
        in_specs=[hbm] * 4,
        out_specs=hbm,
        scratch_shapes=[
            pltpu.VMEM((heads, block, dk), BF16),
            pltpu.VMEM((heads, block, dk), BF16),
            pltpu.VMEM((heads, block, dv), BF16),
            pltpu.VMEM((block, 128), BF16),
            pltpu.VMEM((heads, block, 128), F32),
            pltpu.VMEM((heads, 1, block), F32),
            pltpu.VMEM((blocks, heads, dv), F32),
            pltpu.VMEM((3 * steps + 3, heads, dv), F32),
            pltpu.VMEM((block, block), BF16),
            pltpu.VMEM((units, urows, dv), F32),
            pltpu.VMEM((units, urows, dv), F32),
            pltpu.VMEM((heads, block, dv), F32),
            pltpu.VMEM((units, urows, dv), BF16),
            pltpu.VMEM((heads, block, dv), BF16),
            pltpu.VMEM((hops, units, urows, dv), BF16),
            pltpu.VMEM((hops, units, urows, dv), BF16),
            pltpu.VMEM((units, urows, dv), BF16),
            pltpu.VMEM((units, urows, dv), BF16),
            pltpu.VMEM((units, urows, dv), BF16),
            pltpu.VMEM((units, urows, dv), BF16),
            dma(4, heads), dma(4, heads), dma(4, heads),
            dma(blocks), dma(blocks),
            dma(hops, units), dma(hops, units),
            dma(units), dma(units), dma(units), dma(units),
            dma(heads), dma(heads), dma(heads),
        ],
        compiler_params=pltpu.CompilerParams(
            collective_id=0, has_side_effects=True, vmem_limit_bytes=67043328
        ),
    )(queries, key_vectors, values, dec)
    spec = pl.BlockSpec((rows, dv), lambda i: (0, i))
    return pl.pallas_call(
        gate_kernel,
        out_shape=jax.ShapeDtypeStruct(values.shape, BF16),
        grid=(head_count,),
        in_specs=[spec, spec],
        out_specs=spec,
    )(retained, gate_input)


def solution(mesh):
    spec = P(("seq", "head"), None)
    fn = functools.partial(shards, mesh.shape["seq"], mesh.shape["head"])
    return jax.shard_map(fn, mesh=mesh, in_specs=(spec,) * 5, out_specs=spec, check_vma=False)
```

```python
import functools

import jax
import jax.numpy as jnp
from jax import lax
from jax.experimental import pallas as pl
from jax.experimental.pallas import tpu as pltpu
from jax.sharding import PartitionSpec as P

MESH = pl.DeviceIdType.MESH
F32 = jnp.float32
BF16 = jnp.bfloat16
LAG = 3
CUTS = 4
TILE = 64


def dot(a, b, dims):
    return lax.dot_general(a, b, (dims, ((), ())), preferred_element_type=F32)


def wide(column, times):
    return jnp.concatenate([column] * times, axis=1)


def retention_kernel(
    seqs, chips, heads, q_ref, k_ref, v_ref, dec_ref, out_ref,
    qbuf, kbuf, vbuf, decbuf, runcol, runrow, gath, coef, tri,
    abuf, ebuf, within, slow, retbuf, sbuf, rbuf, supb, rupb, sdnb, rdnb,
    xs, xr, loc, gs, gr, ss, sr, ups, upr, dns, dnr, rets, retr, retl,
):
    s = lax.axis_index("seq")
    h = lax.axis_index("head")
    c = lax.rem(h, 2)
    z = h // 2
    steps = seqs.bit_length() - 1
    rows = q_ref.shape[0]
    block = 2 * rows
    dk = qbuf.shape[2]
    dv = vbuf.shape[2]
    blocks = seqs * chips
    me = s * chips + z
    units = heads * CUTS
    urows = dk // CUTS
    mate = {"seq": s, "head": h + 1 - 2 * c}

    def spot(b):
        return {"seq": b // chips, "head": 2 * lax.rem(b, chips) + c}

    barrier = pltpu.get_barrier_semaphore()
    pl.semaphore_signal(barrier, inc=1, device_id=mate, device_id_type=MESH)

    def greet(o, _):
        pl.semaphore_signal(
            barrier, inc=1, device_id=spot(lax.rem(me + o, blocks)), device_id_type=MESH
        )
        return 0

    lax.fori_loop(1, blocks, greet, 0)
    mine = pl.ds(pl.multiple_of(c * rows, rows), rows)

    def swap(kind, i):
        if kind == 3:
            source, target = dec_ref, decbuf.at[mine]
        else:
            ref, buf = ((k_ref, kbuf), (v_ref, vbuf), (q_ref, qbuf))[kind]
            width = buf.shape[2]
            col = pl.multiple_of(((1 - c) * heads + i) * width, width)
            source, target = ref.at[:, pl.ds(col, width)], buf.at[i, mine, :]
        return pltpu.make_async_remote_copy(
            src_ref=source, dst_ref=target, send_sem=xs.at[kind, i], recv_sem=xr.at[kind, i],
            device_id=mate, device_id_type=MESH,
        )

    def keep(kind, i):
        ref, buf = ((k_ref, kbuf), (v_ref, vbuf), (q_ref, qbuf))[kind]
        width = buf.shape[2]
        col = pl.multiple_of((c * heads + i) * width, width)
        source, target = ref.at[:, pl.ds(col, width)], buf.at[i, mine, :]
        return pltpu.make_async_copy(source, target, loc.at[kind, i])

    def launch(i, _):
        for kind in (0, 1):
            keep(kind, i).start()
        return 0

    lax.fori_loop(0, heads, launch, 0)
    row_id = lax.broadcasted_iota(jnp.int32, (block, block), 0)
    col_id = lax.broadcasted_iota(jnp.int32, (block, block), 1)
    tri[...] = jnp.where(row_id >= col_id, 1.0, 0.0).astype(BF16)
    decbuf[mine] = dec_ref[...]
    pl.semaphore_wait(barrier, blocks)
    swap(3, 0).start()

    def launch_swap(i, _):
        for kind in (0, 1):
            swap(kind, i).start()
        return 0

    lax.fori_loop(0, heads, launch_swap, 0)

    def launch_q(i, _):
        swap(2, i).start()
        keep(2, i).start()
        return 0

    lax.fori_loop(0, heads, launch_q, 0)
    swap(3, 0).wait_recv()
    dec = decbuf[...]
    running = dot(tri[...], dec, ((1,), (0,)))
    run_rows = dot(dec, tri[...], ((0,), (1,)))
    running = jnp.where(c == 0, running[:, :heads], running[:, heads:])
    run_rows = jnp.where(c == 0, run_rows[:heads, :], run_rows[heads:, :])
    totals = dot(dec, jnp.ones((block, dv), BF16), ((0,), (0,)))
    gath[me] = jnp.where(c == 0, totals[:heads, :], totals[heads:, :])
    runrow[...] = run_rows[:, None, :]
    for i in range(heads):
        runcol[i] = jnp.broadcast_to(running[:, i : i + 1], (block, 128))

    def tell(o, where):
        return pltpu.make_async_remote_copy(
            src_ref=gath.at[me], dst_ref=gath.at[where], send_sem=gs.at[o], recv_sem=gr.at[o],
            device_id=spot(lax.rem(me + o, blocks)), device_id_type=MESH,
        )

    def tell_start(o, _):
        tell(o, me).start()
        return 0

    lax.fori_loop(1, blocks, tell_start, 0)

    def hop(k, u):
        other = s ^ (1 << k)
        return pltpu.make_async_remote_copy(
            src_ref=sbuf.at[k, u], dst_ref=rbuf.at[k, u], send_sem=ss.at[k, u],
            recv_sem=sr.at[k, u], device_id={"seq": other, "head": h}, device_id_type=MESH,
        )

    def up(u):
        return pltpu.make_async_remote_copy(
            src_ref=supb.at[u], dst_ref=rupb.at[u], send_sem=ups.at[u], recv_sem=upr.at[u],
            device_id={"seq": s, "head": lax.rem(h + 2, 2 * chips)}, device_id_type=MESH,
        )

    def down(u):
        return pltpu.make_async_remote_copy(
            src_ref=sdnb.at[u], dst_ref=rdnb.at[u], send_sem=dns.at[u], recv_sem=dnr.at[u],
            device_id={"seq": s, "head": lax.rem(h - 2 + 2 * chips, 2 * chips)},
            device_id_type=MESH,
        )

    def bit(k):
        return lax.rem(s // (1 << k), 2)

    def sends(k):
        return True if k < steps - 1 else bit(k) == 0

    def gets(k):
        return True if k < steps - 1 else bit(k) == 1

    def state(i, _):
        for kind in (0, 1):
            keep(kind, i).wait()
            swap(kind, i).wait_recv()
        total = gath[me, pl.ds(i, 1), :][:, :128]
        fade = wide(jnp.exp(total - runcol[i]), dk // 128)
        faded = (kbuf[i].astype(F32) * fade).astype(BF16)
        for cut in range(CUTS):
            u = i * CUTS + cut
            part = dot(faded[:, cut * urows : (cut + 1) * urows], vbuf[i], ((0,), (0,)))
            abuf[u] = part
            if steps > 0:
                sbuf[0, u] = part.astype(BF16)

                @pl.when(sends(0))
                def _():
                    hop(0, u).start()

        return 0

    lax.fori_loop(0, heads, state, 0)

    def hear(o, _):
        tell(o, lax.rem(me - o + blocks, blocks)).wait_recv()
        return 0

    lax.fori_loop(1, blocks, hear, 0)

    def span(slot, lo, hi, live=None):
        total = lax.fori_loop(
            lo, hi, lambda b, acc: acc + gath[b], jnp.zeros((heads, dv), F32)
        )
        value = jnp.exp(total)
        if live is not None:
            value = value * live.astype(F32)
        coef[slot] = value

    def end(p, k):
        return p * chips + z + 1 if k == 0 else (p // (1 << k) + 1) * (1 << k) * chips

    for k in range(steps):
        other = s ^ (1 << k)
        span(3 * k, end(s, k), end(s, k + 1))
        span(3 * k + 1, end(other, k), end(s, k + 1))
        span(3 * k + 2, end(other, k), jnp.maximum(s * chips, end(other, k)), bit(k))
    base = 3 * steps
    span(base, me, me + 1)
    span(base + 1, s * chips, me + 1)
    span(base + 2, s * chips, me)

    @pl.when(z == 0)
    def _():
        rupb[...] = jnp.zeros(rupb.shape, BF16)

    @pl.when(z == chips - 1)
    def _():
        rdnb[...] = jnp.zeros(rdnb.shape, BF16)

    def scale(slot, u):
        return coef[slot, pl.ds(u // CUTS, 1), :]

    def when(live, u, fn):
        pl.when(jnp.logical_and(live, jnp.logical_and(u >= 0, u < units)))(lambda: fn(u))

    def step(t, _):
        for k in range(steps):

            def scan(u, k=k):
                @pl.when(gets(k))
                def _():
                    hop(k, u).wait_recv()
                    got = rbuf[k, u].astype(F32)
                    add = got * scale(3 * k + 2, u)
                    ebuf[u] = add if k == 0 else ebuf[u] + add
                    if k < steps - 1:
                        own = abuf[u] if k == 0 else sbuf[k, u].astype(F32)
                        sbuf[k + 1, u] = (
                            own * scale(3 * k, u) + got * scale(3 * k + 1, u)
                        ).astype(BF16)

                if k == 0 and steps == 1:

                    @pl.when(jnp.logical_not(gets(0)))
                    def _():
                        ebuf[u] = jnp.zeros((urows, dv), F32)

                if k < steps - 1:

                    @pl.when(sends(k + 1))
                    def _():
                        hop(k + 1, u).start()

            when(True, t - LAG * k, scan)
        if steps == 0:

            def blank(u):
                ebuf[u] = jnp.zeros((urows, dv), F32)

            when(True, t, blank)
        ready = t - LAG * max(steps - 1, 0)

        def rise(u):
            @pl.when(z > 0)
            def _():
                up(u).wait_recv()

            @pl.when(z < chips - 1)
            def _():
                supb[u] = (
                    rupb[u].astype(F32) * scale(base, u)
                    + abuf[u]
                    + scale(base + 1, u) * ebuf[u]
                ).astype(BF16)
                up(u).start()

        when(True, ready - LAG * z, rise)

        def sink(u):
            @pl.when(z < chips - 1)
            def _():
                down(u).wait_recv()

            @pl.when(z > 0)
            def _():
                sdnb[u] = (rdnb[u].astype(F32) + ebuf[u]).astype(BF16)
                down(u).start()

        when(True, ready - LAG * (chips - 1 - z), sink)

        def local(i):
            keep(2, i).wait()
            swap(2, i).wait_recv()
            scores = dot(qbuf[i], kbuf[i], ((1,), (1,)))
            spread = wide(runcol[i], block // 128) - runrow[i]
            row = lax.broadcasted_iota(jnp.int32, (block, block), 0)
            col = lax.broadcasted_iota(jnp.int32, (block, block), 1)
            factor = jnp.exp(jnp.where(row >= col, spread, -jnp.inf))
            weights = (scores * factor).astype(BF16)
            within[i] = dot(weights, vbuf[i], ((1,), (0,)))

        pl.when(jnp.logical_and(lax.rem(t, CUTS) == 0, t < units))(lambda: local(t // CUTS))

        def finish(u):
            i = u // CUTS
            start = rupb[u].astype(F32) + scale(base + 2, u) * (rdnb[u].astype(F32) + ebuf[u])
            slow[u] = start.astype(BF16)

            @pl.when(lax.rem(u, CUTS) == CUTS - 1)
            def _():
                low = slow[pl.ds(i * CUTS, CUTS)].reshape(dk, dv)
                across = dot(qbuf[i], low, ((1,), (0,)))
                across = across * wide(jnp.exp(runcol[i]), dv // 128)
                retbuf[i] = (within[i] + across).astype(BF16)
                give(i).start()
                stay(i).start()

        when(True, ready - LAG * jnp.maximum(z, chips - 1 - z), finish)
        return 0

    yours = pl.ds(pl.multiple_of((1 - c) * rows, rows), rows)

    def give(i):
        col = pl.multiple_of((c * heads + i) * dv, dv)
        return pltpu.make_async_remote_copy(
            src_ref=retbuf.at[i, yours, :], dst_ref=out_ref.at[:, pl.ds(col, dv)],
            send_sem=rets.at[i], recv_sem=retr.at[i], device_id=mate, device_id_type=MESH,
        )

    def take(i):
        col = pl.multiple_of(((1 - c) * heads + i) * dv, dv)
        return pltpu.make_async_remote_copy(
            src_ref=retbuf.at[i, yours, :], dst_ref=out_ref.at[:, pl.ds(col, dv)],
            send_sem=rets.at[i], recv_sem=retr.at[i], device_id=mate, device_id_type=MESH,
        )

    def stay(i):
        col = pl.multiple_of((c * heads + i) * dv, dv)
        return pltpu.make_async_copy(
            retbuf.at[i, mine, :], out_ref.at[:, pl.ds(col, dv)], retl.at[i]
        )

    total_steps = units + LAG * max(steps - 1, 0) + LAG * (chips - 1)
    lax.fori_loop(0, total_steps, step, 0)

    swap(3, 0).wait_send()

    def close(i, _):
        for kind in range(3):
            swap(kind, i).wait_send()
        give(i).wait_send()
        take(i).wait_recv()
        stay(i).wait()
        return 0

    lax.fori_loop(0, heads, close, 0)

    def close_tell(o, _):
        tell(o, me).wait_send()
        return 0

    lax.fori_loop(1, blocks, close_tell, 0)

    def close_units(u, _):
        for k in range(steps):

            @pl.when(sends(k))
            def _():
                hop(k, u).wait_send()

        @pl.when(z < chips - 1)
        def _():
            up(u).wait_send()

        @pl.when(z > 0)
        def _():
            down(u).wait_send()

        return 0

    lax.fori_loop(0, units, close_units, 0)


def gate_kernel(heads, ret_ref, gate_ref, out_ref):
    width = ret_ref.shape[1] // heads
    for i in range(heads):
        part = pl.ds(i * width, width)
        kept = ret_ref[:, part].astype(F32)
        centered = kept - jnp.mean(kept, axis=1, keepdims=True)
        variance = jnp.mean(centered * centered, axis=1, keepdims=True)
        gate = gate_ref[:, part].astype(F32)
        half = 0.5 * gate
        swish = half + half * jnp.tanh(half)
        out_ref[:, part] = (swish * (centered * lax.rsqrt(variance + 1e-06))).astype(BF16)


def shards(seqs, groups, queries, key_vectors, values, decay_log, gate_input):
    rows, head_count = decay_log.shape
    heads = head_count // 2
    chips = groups // 2
    dk = queries.shape[1] // head_count
    dv = values.shape[1] // head_count
    block = 2 * rows
    blocks = seqs * chips
    units = heads * CUTS
    urows = dk // CUTS
    steps = seqs.bit_length() - 1
    hops = max(steps, 1)
    hbm = pl.BlockSpec(memory_space=pl.ANY)
    dma = lambda *shape: pltpu.SemaphoreType.DMA(shape)
    retained = pl.pallas_call(
        functools.partial(retention_kernel, seqs, chips, heads),
        out_shape=jax.ShapeDtypeStruct(values.shape, BF16),
        in_specs=[hbm] * 3 + [pl.BlockSpec(memory_space=pltpu.VMEM)],
        out_specs=hbm,
        scratch_shapes=[
            pltpu.VMEM((heads, block, dk), BF16),
            pltpu.VMEM((heads, block, dk), BF16),
            pltpu.VMEM((heads, block, dv), BF16),
            pltpu.VMEM((block, head_count), BF16),
            pltpu.VMEM((heads, block, 128), F32),
            pltpu.VMEM((heads, 1, block), F32),
            pltpu.VMEM((blocks, heads, dv), F32),
            pltpu.VMEM((3 * steps + 3, heads, dv), F32),
            pltpu.VMEM((block, block), BF16),
            pltpu.VMEM((units, urows, dv), F32),
            pltpu.VMEM((units, urows, dv), F32),
            pltpu.VMEM((heads, block, dv), F32),
            pltpu.VMEM((units, urows, dv), BF16),
            pltpu.VMEM((heads, block, dv), BF16),
            pltpu.VMEM((hops, units, urows, dv), BF16),
            pltpu.VMEM((hops, units, urows, dv), BF16),
            pltpu.VMEM((units, urows, dv), BF16),
            pltpu.VMEM((units, urows, dv), BF16),
            pltpu.VMEM((units, urows, dv), BF16),
            pltpu.VMEM((units, urows, dv), BF16),
            dma(4, heads), dma(4, heads), dma(4, heads),
            dma(blocks), dma(blocks),
            dma(hops, units), dma(hops, units),
            dma(units), dma(units), dma(units), dma(units),
            dma(heads), dma(heads), dma(heads),
        ],
        compiler_params=pltpu.CompilerParams(
            collective_id=0, has_side_effects=True, vmem_limit_bytes=67043328
        ),
    )(queries, key_vectors, values, decay_log)
    tile = min(TILE, rows)
    spec = pl.BlockSpec((tile, values.shape[1]), lambda i: (i, 0))
    return pl.pallas_call(
        functools.partial(gate_kernel, head_count),
        out_shape=jax.ShapeDtypeStruct(values.shape, BF16),
        grid=(rows // tile,),
        in_specs=[spec, spec],
        out_specs=spec,
    )(retained, gate_input)


def solution(mesh):
    spec = P(("seq", "head"), None)
    fn = functools.partial(shards, mesh.shape["seq"], mesh.shape["head"])
    return jax.shard_map(fn, mesh=mesh, in_specs=(spec,) * 5, out_specs=spec, check_vma=False)
```
